32 devices in a mesh: dp: 8 (over z, y), section: 4 (over x, core).
Axes of the slice: x: 2, y: 2, z: 4, core: 2. Of those that a mesh axis runs over, the one named last changes fastest.
Arguments:
- patches: bfloat16 [64, 197, 1024], P('dp'), may hold values from -6 to 6
- ln1_gain: float32 [4, 1024], P('section'), may hold values from 0.5 to 1.5
- w_qkv: bfloat16 [4, 1024, 3072], P('section'), may hold values from -1 to 1
- w_out: bfloat16 [4, 1024, 1024], P('section'), may hold values from -0.1875 to 0.1875
- ln2_gain: float32 [4, 1024], P('section'), may hold values from 0.5 to 1.5
- w_fc1: bfloat16 [4, 1024, 2048], P('section'), may hold values from -0.1875 to 0.1875
- w_fc2: bfloat16 [4, 2048, 1024], P('section'), may hold values from -0.125 to 0.125
- final_norm_gain: float32 [1024], replicated, may hold values from 0.5 to 1.5
- w_head: bfloat16 [1024, 256], replicated, may hold values from -0.1875 to 0.1875
- online_embeddings: bfloat16 [64, 256], P('dp'), may hold values from -60 to 60
- queue: bfloat16 [32768, 256], P(('dp', 'section')), may hold values from -1 to 1, as said below
- owner: int32 [64], replicated, may hold values from 0 to 63, each once
- pointer: int32 [8], P('dp'), may hold values from 0 to 4088
Outputs:
- momentum_embeddings: bfloat16 [64, 256], P('dp')
- query_loss: float32 [64], P('dp')
- total_loss: float32 [], replicated
- new_queue: bfloat16 [32768, 256], P(('dp', 'section'))
The draws below stay inside these ranges and needn't reach their ends.
Inputs may be any that keep to these rules, and one draw needn't show every extreme that they name: `queue`: every row has Euclidean norm below 1. Each value appears once: key j goes to group owner[j] // 8, so every group receives exactly 8 keys. `pointer`: first row of the group's shard where its new keys are written.
All inputs are finite; a program needn't handle non-finite values.
Results may differ from the reference program's by a relative error of at most 0.02.
Values may be sent and summed in bfloat16 or wider, within the bound.
A program may use at most 128 MiB of HBM per device.

```python
import math
import jax
import jax.numpy as jnp
from jax import lax

D = 1024
HEADS = 16
HEAD_DIM = 64
FF = 2048
TOKS = 197
KDIM = 256
Q_GROUP = 4096
IMG_GROUP = 8
IMAGES = 64
QROWS = 32768
N_DP = 8
N_SECTION = 4


def draw_w_qkv(key, part):
    result = jax.random.normal(jax.random.fold_in(key, 23), (N_SECTION, D, 3 * D), jnp.float32) / D ** 0.5
    result = jnp.clip(result, -6.0 / D ** 0.5, 6.0 / D ** 0.5)
    return result.astype(jnp.bfloat16)


def queue_rows(key):
    sample_count = jax.random.normal(jax.random.fold_in(key, 11), (QROWS, KDIM), jnp.float32)
    return sample_count * jax.lax.rsqrt(jnp.sum(sample_count * sample_count, axis=1, keepdims=True) + 1.0)


def draw_queue(key, part):
    return queue_rows(key).astype(jnp.bfloat16)


def draw_online_embeddings(key, part):
    result = jnp.clip(jax.random.normal(jax.random.fold_in(key, 5), (IMAGES, KDIM), jnp.float32), -6.0, 6.0)
    return result.astype(jnp.bfloat16)


def plant(drawn, key, low, largest):
    place = [jax.random.randint(jax.random.fold_in(key, axis), (), 0, length) for axis, length in enumerate(drawn.shape)]
    main_axis = drawn.shape.index(max(drawn.shape))
    beside = place[:main_axis] + [(place[main_axis] + 1) % drawn.shape[main_axis]] + place[main_axis + 1:]
    return drawn.at[tuple(place)].set(low).at[tuple(beside)].set(largest)


def block_levels(key, shape, cuts, least, top_value):
    level = 1.0
    for position, blocks in cuts:
        heights = jax.random.uniform(jax.random.fold_in(jax.random.fold_in(key, 6), position), (blocks,), jnp.float32, least / len(cuts), top_value / len(cuts))
        level = level * jnp.repeat(jnp.exp(heights), shape[position] // blocks).reshape((-1,) + (1,) * (len(shape) - 1 - position))
    return level


def scatter_about(key, dims, scale, limit, cuts=(), kind=jnp.bfloat16):
    loudness = block_levels(key, dims, cuts, -0.22, 0.18) if cuts else 1.0
    array = jax.random.normal(key, dims, jnp.float32) * scale * loudness
    return jnp.minimum(jnp.maximum(array, -limit), limit).astype(kind)


def setup_inputs(seed: int = 0) -> dict:
    seeds = jax.random.split(jax.random.key(seed), 14)
    return {
        "patches": scatter_about(seeds[0], (IMAGES, TOKS, D), 1.0, 6.0, ((0, 8),)),
        "ln1_gain": jnp.clip(1.0 + 0.1 * jax.random.normal(seeds[1], (N_SECTION, D), jnp.float32), 0.5, 1.5),
        "w_qkv": draw_w_qkv(jax.random.fold_in(seeds[13], 71), 0),
        "w_out": scatter_about(seeds[3], (N_SECTION, D, D), D ** -0.5, 0.1875, ((0, 4),)),
        "ln2_gain": jnp.clip(1.0 + 0.1 * jax.random.normal(seeds[4], (N_SECTION, D), jnp.float32), 0.5, 1.5),
        "w_fc1": scatter_about(seeds[5], (N_SECTION, D, FF), D ** -0.5, 0.1875, ((0, 4),)),
        "w_fc2": scatter_about(seeds[6], (N_SECTION, FF, D), FF ** -0.5, 0.125, ((0, 4),)),
        "final_norm_gain": jnp.clip(1.0 + 0.1 * jax.random.normal(seeds[7], (D,), jnp.float32), 0.5, 1.5),
        "w_head": scatter_about(seeds[8], (D, KDIM), D ** -0.5, 0.1875),
        "online_embeddings": draw_online_embeddings(jax.random.fold_in(seeds[13], 71), 0),
        "queue": draw_queue(jax.random.fold_in(seeds[13], 71), 0),
        "owner": jax.random.permutation(seeds[11], IMAGES).astype(jnp.int32),
        "pointer": plant(jax.random.randint(seeds[12], (N_DP,), 0, Q_GROUP - IMG_GROUP + 1), jax.random.fold_in(seeds[12], 1), 0, Q_GROUP - IMG_GROUP).astype(jnp.int32),
    }


contrastive_sharpness = 0.2

def layer_norm(values, gain):
    center = values - lax.optimization_barrier(jnp.mean(values, axis=-1, keepdims=True))
    spread = lax.optimization_barrier(jnp.mean(center * center, axis=-1, keepdims=True))
    return center * lax.rsqrt(spread + 1e-06) * gain

def cycle_buffer(values):
    return lax.optimization_barrier(values.astype(jnp.bfloat16)).astype(jnp.float32)

def encoder_block(hidden, gain_one, qkv_weight, out_weight, gain_two, first_weight, second_weight):
    images = hidden.shape[0]
    width = hidden.shape[2]
    stream = hidden.astype(jnp.float32)
    normed = layer_norm(stream, gain_one).astype(jnp.bfloat16).reshape(images * TOKS, width)
    packed = jnp.dot(normed, qkv_weight, preferred_element_type=jnp.float32)
    packed = cycle_buffer(packed).reshape(images, TOKS, 3, HEADS, HEAD_DIM)
    similarity_matrix = jnp.einsum('bqhd,bkhd->bhqk', packed[:, :, 0], packed[:, :, 1]) / math.sqrt(HEAD_DIM)
    peak = lax.optimization_barrier(jnp.max(similarity_matrix, axis=-1, keepdims=True))
    expo = jnp.exp(similarity_matrix - peak)
    probs = cycle_buffer(expo / lax.optimization_barrier(jnp.sum(expo, axis=-1, keepdims=True)))
    context = jnp.einsum('bhqk,bkhd->bqhd', probs, packed[:, :, 2])
    context = context.astype(jnp.bfloat16).reshape(images * TOKS, width)
    stream = stream + jnp.dot(context, out_weight, preferred_element_type=jnp.float32).reshape(images, TOKS, width)
    normed = layer_norm(stream, gain_two).astype(jnp.bfloat16).reshape(images * TOKS, width)
    inner = jax.nn.gelu(jnp.dot(normed, first_weight, preferred_element_type=jnp.float32), approximate=False)
    inner = inner.astype(jnp.bfloat16)
    stream = stream + jnp.dot(inner, second_weight, preferred_element_type=jnp.float32).reshape(images, TOKS, width)
    return stream.astype(jnp.bfloat16)

def key_head(class_rows, final_norm_gain, w_head):
    normed = layer_norm(class_rows.astype(jnp.float32), final_norm_gain).astype(jnp.bfloat16)
    projected = jnp.dot(normed, w_head, preferred_element_type=jnp.float32)
    scale = lax.rsqrt(1.0 + lax.optimization_barrier(jnp.sum(projected * projected, axis=1, keepdims=True)))
    return (projected * scale).astype(jnp.bfloat16)

def reference(patches, ln1_gain, w_qkv, w_out, ln2_gain, w_fc1, w_fc2, final_norm_gain, w_head, online_embeddings, queue, owner, pointer):

    def encode_group(images):
        hidden = images
        for layer_section in range(N_SECTION):
            hidden = encoder_block(hidden, ln1_gain[layer_section], w_qkv[layer_section], w_out[layer_section], ln2_gain[layer_section], w_fc1[layer_section], w_fc2[layer_section])
        return key_head(hidden[:, 0, :], final_norm_gain, w_head)
    momentum_embeddings = lax.map(encode_group, patches.reshape(N_DP, IMG_GROUP, TOKS, D)).reshape(IMAGES, KDIM)
    matching_similarity = lax.optimization_barrier(jnp.sum(online_embeddings.astype(jnp.float32) * momentum_embeddings.astype(jnp.float32), axis=1)) / contrastive_sharpness

    def score_group(sample_count):
        similarity_matrix = jnp.dot(online_embeddings, sample_count.T, preferred_element_type=jnp.float32) / contrastive_sharpness
        peak = lax.optimization_barrier(jnp.max(similarity_matrix, axis=1))
        return (peak, lax.optimization_barrier(jnp.sum(jnp.exp(similarity_matrix - peak[:, None]), axis=1)))
    peaks, totals = lax.map(score_group, queue.reshape(N_DP, Q_GROUP, KDIM))
    top = lax.optimization_barrier(jnp.max(peaks, axis=0))
    negative = top + jnp.log(lax.optimization_barrier(jnp.sum(totals * jnp.exp(peaks - top[None, :]), axis=0)))
    larger = jnp.maximum(negative, matching_similarity)
    query_loss = larger + jnp.log(jnp.exp(negative - larger) + jnp.exp(matching_similarity - larger)) - matching_similarity
    total_loss = jnp.sum(query_loss) / IMAGES
    order = jnp.zeros((IMAGES,), jnp.int32).at[owner].set(jnp.arange(IMAGES, dtype=jnp.int32))
    entries = momentum_embeddings[order].reshape(N_DP, IMG_GROUP, KDIM)

    def enqueue(pieces):
        sample_count, fresh, start = pieces
        return lax.dynamic_update_slice_in_dim(sample_count, fresh, start.astype(jnp.int32), 0)
    new_queue = lax.map(enqueue, (queue.reshape(N_DP, Q_GROUP, KDIM), entries, pointer)).reshape(QROWS, KDIM)
    return (momentum_embeddings, query_loss, total_loss, new_queue)
```

```python
import functools
import math

import jax
import jax.numpy as jnp
from jax import lax
from jax.experimental import pallas as pl
from jax.experimental.pallas import tpu as pltpu
from jax.sharding import PartitionSpec as P

HEAD_DIM = 64
LANES = 128
SHARPNESS = 0.2
f32 = jnp.float32
bf16 = jnp.bfloat16
MESH = pl.DeviceIdType.MESH


def layer_norm(values, gain):
    center = values - jnp.mean(values, axis=-1, keepdims=True)
    spread = jnp.mean(center * center, axis=-1, keepdims=True)
    return center * lax.rsqrt(spread + 1e-06) * gain


def rounded_up(value, step):
    return (value + step - 1) // step * step


def gelu(x):
    return 0.5 * x * (1.0 + lax.erf(x * math.sqrt(0.5)))


def dot(a, b):
    return jnp.dot(a, b, preferred_element_type=f32)


def dot_nt(a, b):
    return lax.dot_general(a, b, (((1,), (1,)), ((), ())), preferred_element_type=f32)


def column_loop(total, tile, body):
    for at in range(0, total, tile):
        body(at, tile)


def attend(qkv_buf, c_buf, toks, width):
    rows = c_buf.shape[0]
    pair = 2 * HEAD_DIM
    lane = lax.broadcasted_iota(jnp.int32, (rows, pair), 1)
    place = lax.broadcasted_iota(jnp.int32, (rows, pair), 0)
    first = lane < HEAD_DIM
    factor = math.log2(math.e) / math.sqrt(HEAD_DIM)
    one = (place < toks).astype(f32).astype(bf16)
    for at in range(0, width, pair):
        q = qkv_buf[:, pl.ds(at, pair)]
        zero = jnp.zeros_like(q)
        q_both = jnp.concatenate([jnp.where(first, q, zero), jnp.where(first, zero, q)], axis=0)
        scores = dot_nt(q_both, qkv_buf[:, pl.ds(width + at, pair)])
        peak = jnp.max(scores, axis=1, keepdims=True)
        expo = jnp.exp2((scores - peak) * factor)
        v_and_one = jnp.concatenate([qkv_buf[:, pl.ds(2 * width + at, pair)], one], axis=1)
        c = dot(expo.astype(bf16), v_and_one)
        above = jnp.where(first, c[:rows, :pair], c[rows:, :pair])
        below = jnp.where(first, c[:rows, pair:], c[rows:, pair:])
        c_buf[:, pl.ds(at, pair)] = (above / below).astype(bf16)


def encoder_kernel(
    sections,
    groups,
    toks,
    patches,
    online,
    gain_one,
    gain_two,
    gain_last,
    w_qkv,
    w_out,
    w_fc1,
    w_fc2,
    w_head,
    queue,
    owner,
    pointer,
    keys_out,
    loss_out,
    total_out,
    queue_out,
    v_qkv,
    v_out,
    v_fc1,
    v_fc2,
    v_head,
    raw,
    flat,
    came,
    leaving,
    a_buf,
    qkv_buf,
    c_buf,
    r_buf,
    u_buf,
    row_h,
    row_c,
    q_buf,
    code_buf,
    place_buf,
    stat_buf,
    stat_recv,
    key_buf,
    loss_buf,
    weight_sem,
    raw_sem,
    send_sem,
    recv_sem,
    q_send,
    q_recv,
    stat_send_sem,
    stat_recv_sem,
    key_send,
    key_recv,
    loss_send,
    loss_recv,
):
    me = lax.axis_index("section")
    group = lax.axis_index("dp")
    images, rows, width = came.shape
    hidden = v_fc1.shape[1]
    share, kdim = queue.shape
    last = sections - 1
    devices = groups * sections
    own = group * sections + me
    part = width // 2
    n_parts = 3 * width // part

    raw_load = pltpu.make_async_copy(patches, raw, raw_sem)
    qkv_loads = [
        pltpu.make_async_copy(
            w_qkv.at[0, :, pl.ds(i * part, part)],
            v_qkv.at[:, pl.ds(i * part, part)],
            weight_sem.at[i],
        )
        for i in range(n_parts)
    ]
    other_loads = [
        pltpu.make_async_copy(source, target, weight_sem.at[n_parts + i])
        for i, (source, target) in enumerate(
            ((w_out.at[0], v_out), (w_fc1.at[0], v_fc1), (w_fc2.at[0], v_fc2))
        )
    ]
    head_load = pltpu.make_async_copy(w_head, v_head, weight_sem.at[n_parts + 3])

    @pl.when(me == 0)
    def _():
        raw_load.start()

    for load in qkv_loads + other_loads:
        load.start()

    @pl.when(me == last)
    def _():
        head_load.start()

    barrier = pltpu.get_barrier_semaphore()

    @pl.loop(1, devices)
    def _(step):
        there = lax.rem(own + step, devices)
        pl.semaphore_signal(
            barrier,
            inc=1,
            device_id={"dp": there // sections, "section": lax.rem(there, sections)},
            device_id_type=MESH,
        )

    def query_copy(step):
        return pltpu.make_async_remote_copy(
            src_ref=online,
            dst_ref=q_buf.at[group],
            send_sem=q_send.at[step],
            recv_sem=q_recv.at[step],
            device_id={"dp": lax.rem(group + step, groups)},
            device_id_type=MESH,
        )

    def enter():
        pl.semaphore_wait(barrier, devices - 1)
        for step in range(1, groups):
            query_copy(step).start()

    def stat_copy(step):
        there = lax.rem(group + step, groups)
        return pltpu.make_async_remote_copy(
            src_ref=stat_buf.at[there],
            dst_ref=stat_recv.at[own],
            send_sem=stat_send_sem.at[step],
            recv_sem=stat_recv_sem.at[own],
            device_id={"dp": there, "section": last},
            device_id_type=MESH,
        )

    def side_work():
        for step in range(1, groups):
            query_copy(step).wait()
        q_buf[group] = online[...]
        queries = q_buf[...].astype(f32).reshape(groups * images, kdim).astype(bf16)
        scores = dot_nt(queries, queue[...]) / SHARPNESS
        peak = jnp.max(scores, axis=1, keepdims=True)
        total = jnp.sum(jnp.exp(scores - peak), axis=1, keepdims=True)
        stat = jnp.broadcast_to(peak + jnp.log(total), (groups * images, LANES))
        stat_buf[...] = stat.reshape(groups, images, LANES)

        for step in range(1, groups):
            stat_copy(step).start()

        @pl.when(me < last)
        def _():
            stat_copy(0).start()

        slot = (
            lax.broadcasted_iota(jnp.int32, (share, LANES), 0) + me * share - pointer[0]
        )
        inside = jnp.logical_and(slot >= 0, slot < images)
        code = jnp.where(inside, slot + group * images, -1)
        code_buf[...] = code
        place_buf[...] = (code[:, : groups * images] == owner[...]).astype(f32).astype(bf16)

        for step in range(1, groups):
            stat_copy(step).wait_send()

        @pl.when(me < last)
        def _():
            stat_copy(0).wait_send()

    def handing(image):
        return pltpu.make_async_remote_copy(
            src_ref=leaving.at[image],
            dst_ref=came.at[image],
            send_sem=send_sem.at[image],
            recv_sem=recv_sem.at[image],
            device_id={"section": jnp.minimum(me + 1, last)},
            device_id_type=MESH,
        )

    def take(image):
        @pl.when(me == 0)
        def _():
            for tile in range(width // LANES):
                came[image, :, tile * LANES : (tile + 1) * LANES] = flat[
                    tile, pl.ds(image, rows, stride=images), :
                ].astype(bf16)

        @pl.when(me > 0)
        def _():
            handing(image).wait_recv()

    def block(image, starting):
        take(image)
        a_buf[...] = layer_norm(came[image].astype(f32), gain_one[...]).astype(bf16)

        def qkv_part(at, tile):
            if starting:
                qkv_loads[at // tile].wait()
            columns = pl.ds(at, tile)
            qkv_buf[:, columns] = dot(a_buf[...], v_qkv[:, columns]).astype(bf16)

        column_loop(3 * width, part, qkv_part)
        tail = toks // 16 * 16
        kept = lax.broadcasted_iota(jnp.int32, (rows - tail, width), 0) < toks - tail
        end = qkv_buf[tail:, 2 * width :]
        qkv_buf[tail:, 2 * width :] = jnp.where(kept, end, jnp.zeros_like(end))
        if starting:

            @pl.when(me == 0)
            def _():
                enter()

        attend(qkv_buf, c_buf, toks, width)
        if starting:
            other_loads[0].wait()

        def out_part(at, tile):
            columns = pl.ds(at, tile)
            r_buf[:, columns] = came[image, :, columns].astype(f32) + dot(
                c_buf[...], v_out[:, columns]
            )

        column_loop(width, part, out_part)
        a_buf[...] = layer_norm(r_buf[...], gain_two[...]).astype(bf16)
        if starting:
            other_loads[1].wait()

        def fc1_part(at, tile):
            columns = pl.ds(at, tile)
            u_buf[:, columns] = gelu(dot(a_buf[...], v_fc1[:, columns])).astype(bf16)

        column_loop(hidden, part, fc1_part)
        if starting:
            other_loads[2].wait()

        def fc2_part(at, tile):
            columns = pl.ds(at, tile)
            leaving[image, :, columns] = (
                r_buf[:, columns] + dot(u_buf[...], v_fc2[:, columns])
            ).astype(bf16)

        column_loop(width, part, fc2_part)
        handing(image).start()

    def class_row(image):
        handing(image).wait_recv()
        row_h[pl.ds(image, 1), :] = came[image, 0:16, :].astype(f32)[0:1, :]
        a_buf[...] = layer_norm(came[image].astype(f32), gain_one[...]).astype(bf16)
        q = dot(a_buf[0:16, :], v_qkv[:, 0:width]).astype(bf16).astype(f32)[0:1, :]

        def kv_part(at, tile):
            columns = pl.ds(width + at, tile)
            qkv_buf[:, columns] = dot(a_buf[...], v_qkv[:, columns]).astype(bf16)

        column_loop(2 * width, part, kv_part)
        heads = width // HEAD_DIM
        head = lax.broadcasted_iota(jnp.int32, (heads, width), 0)
        lane = lax.broadcasted_iota(jnp.int32, (heads, width), 1)
        mine = lane // HEAD_DIM == head
        spread = jnp.where(mine, jnp.broadcast_to(q, (heads, width)), 0.0).astype(bf16)
        scores = dot_nt(spread, qkv_buf[:, width : 2 * width]) / math.sqrt(HEAD_DIM)
        place = lax.broadcasted_iota(jnp.int32, (heads, rows), 1)
        scores = jnp.where(place < toks, scores, -jnp.inf)
        expo = jnp.exp(scores - jnp.max(scores, axis=1, keepdims=True))
        p = (expo / jnp.sum(expo, axis=1, keepdims=True)).astype(bf16)
        c = dot(p, qkv_buf[:, 2 * width :])
        row_c[pl.ds(image, 1), :] = jnp.sum(jnp.where(mine, c, 0.0), axis=0, keepdims=True)

    def key_copy(step):
        there = lax.rem(own + step, devices)
        return pltpu.make_async_remote_copy(
            src_ref=key_buf.at[group],
            dst_ref=key_buf.at[group],
            send_sem=key_send.at[step],
            recv_sem=key_recv.at[group],
            device_id={"dp": there // sections, "section": lax.rem(there, sections)},
            device_id_type=MESH,
        )

    def loss_copy(step):
        there = lax.rem(own + step, devices)
        return pltpu.make_async_remote_copy(
            src_ref=loss_buf.at[group],
            dst_ref=loss_buf.at[group],
            send_sem=loss_send.at[step],
            recv_sem=loss_recv.at[group],
            device_id={"dp": there // sections, "section": lax.rem(there, sections)},
            device_id_type=MESH,
        )

    def finish_keys():
        r = row_h[...] + dot(row_c[...].astype(bf16), v_out[...])
        u = gelu(dot(layer_norm(r, gain_two[...]).astype(bf16), v_fc1[...])).astype(bf16)
        h = (r + dot(u, v_fc2[...])).astype(bf16).astype(f32)
        z = dot(layer_norm(h, gain_last[...]).astype(bf16), v_head[...])
        keys = (z * lax.rsqrt(1.0 + jnp.sum(z * z, axis=1, keepdims=True))).astype(bf16)
        key_buf[group] = keys

        @pl.loop(1, devices)
        def _(step):
            key_copy(step).start()

        stats = stat_recv[...]
        top = jnp.max(stats, axis=0)
        negative = top + jnp.log(jnp.sum(jnp.exp(stats - top[None]), axis=0))
        positive = jnp.broadcast_to(
            jnp.sum(online[...].astype(f32) * keys.astype(f32), axis=1, keepdims=True) / SHARPNESS,
            (images, LANES),
        )
        larger = jnp.maximum(negative, positive)
        loss = (
            larger + jnp.log(jnp.exp(negative - larger) + jnp.exp(positive - larger)) - positive
        )
        row = lax.broadcasted_iota(jnp.int32, (images, LANES), 0)
        lane = lax.broadcasted_iota(jnp.int32, (images, LANES), 1)
        loss_buf[group] = jnp.sum(jnp.where(row == lane, loss, 0.0), axis=0, keepdims=True)

        @pl.loop(1, devices)
        def _(step):
            loss_copy(step).start()

    @pl.when(me == 0)
    def _():
        raw_load.wait()
        for tile in range(width // LANES):
            columns = slice(tile * LANES, (tile + 1) * LANES)
            flat[tile, 0 : toks * images, :] = (
                raw[:, :, columns].astype(f32).reshape(toks * images, LANES)
            )
            flat[tile, toks * images :, :] = flat[tile, 0 : (rows - toks) * images, :]

    @pl.when(me > 0)
    def _():
        enter()
        side_work()

    @pl.when(me < last)
    def _():
        block(0, True)

        @pl.loop(1, images)
        def _(image):
            block(image, False)

    @pl.when(me == 0)
    def _():
        side_work()

    @pl.when(me == last)
    def _():
        for load in qkv_loads + other_loads + [head_load]:
            load.wait()

        @pl.loop(0, images)
        def _(image):
            class_row(image)

        @pl.loop(1, devices)
        def _(step):
            there = lax.rem(own + step, devices)
            pltpu.make_async_remote_copy(
                src_ref=stat_buf.at[group],
                dst_ref=stat_recv.at[there],
                send_sem=stat_send_sem.at[0],
                recv_sem=stat_recv_sem.at[there],
                device_id={"dp": group, "section": last},
                device_id_type=MESH,
            ).wait_recv()

        stat_recv[own] = stat_buf[group]
        finish_keys()

    for step in range(groups):
        there = lax.rem(group + step, groups)

        def arrived():
            pltpu.make_async_remote_copy(
                src_ref=key_buf.at[there],
                dst_ref=key_buf.at[there],
                send_sem=key_send.at[0],
                recv_sem=key_recv.at[there],
                device_id={"section": last},
                device_id_type=MESH,
            ).wait_recv()
            pltpu.make_async_remote_copy(
                src_ref=loss_buf.at[there],
                dst_ref=loss_buf.at[there],
                send_sem=loss_send.at[0],
                recv_sem=loss_recv.at[there],
                device_id={"section": last},
                device_id_type=MESH,
            ).wait_recv()

        if step == 0:
            pl.when(me < last)(arrived)
        else:
            arrived()

    every_key = key_buf[...].astype(f32).reshape(groups * images, kdim).astype(bf16)
    code = code_buf[...]
    taken = jnp.concatenate([code] * (kdim // LANES), axis=1) >= 0
    queue_out[...] = jnp.where(
        taken, dot(place_buf[...], every_key), queue[...].astype(f32)
    ).astype(bf16)
    keys_out[...] = key_buf[group]
    loss_out[...] = loss_buf[group][:, 0:images]
    losses = jnp.sum(loss_buf[...], axis=0)
    total_out[...] = jnp.sum(losses, axis=1, keepdims=True) / (groups * images)

    @pl.when(me < last)
    def _():
        @pl.loop(0, images)
        def _(image):
            handing(image).wait_send()

    @pl.when(me == last)
    def _():
        @pl.loop(1, devices)
        def _(step):
            key_copy(step).wait_send()
            loss_copy(step).wait_send()


def on_device(
    patches,
    ln1_gain,
    w_qkv,
    w_out,
    ln2_gain,
    w_fc1,
    w_fc2,
    final_norm_gain,
    w_head,
    online_embeddings,
    queue,
    owner,
    pointer,
):
    sections = lax.axis_size("section")
    groups = lax.axis_size("dp")
    devices = sections * groups
    images, toks, width = patches.shape
    rows = rounded_up(toks, 16)
    hidden = w_fc1.shape[2]
    share, kdim = queue.shape
    in_vmem = pl.BlockSpec(memory_space=pltpu.VMEM)
    in_smem = pl.BlockSpec(memory_space=pltpu.SMEM)
    hbm = pl.BlockSpec(memory_space=pl.ANY)
    dma = pltpu.SemaphoreType.DMA
    flops = 2 * images * toks * (4 * width * width + 2 * width * hidden)
    keys, loss, total, new_queue = pl.pallas_call(
        functools.partial(encoder_kernel, sections, groups, toks),
        out_shape=(
            jax.ShapeDtypeStruct((images, kdim), bf16),
            jax.ShapeDtypeStruct((1, images), f32),
            jax.ShapeDtypeStruct((1, 1), f32),
            jax.ShapeDtypeStruct((share, kdim), bf16),
        ),
        in_specs=[hbm] + [in_vmem] * 4 + [hbm] * 5 + [in_vmem] * 2 + [in_smem],
        out_specs=(in_vmem,) * 4,
        scratch_shapes=[
            pltpu.VMEM((width, 3 * width), bf16),
            pltpu.VMEM((width, width), bf16),
            pltpu.VMEM((width, hidden), bf16),
            pltpu.VMEM((hidden, width), bf16),
            pltpu.VMEM((width, kdim), bf16),
            pltpu.VMEM((toks, images, width), bf16),
            pltpu.VMEM((width // LANES, rows * images, LANES), f32),
            pltpu.VMEM((images, rows, width), bf16),
            pltpu.VMEM((images, rows, width), bf16),
            pltpu.VMEM((rows, width), bf16),
            pltpu.VMEM((rows, 3 * width), bf16),
            pltpu.VMEM((rows, width), bf16),
            pltpu.VMEM((rows, width), f32),
            pltpu.VMEM((rows, hidden), bf16),
            pltpu.VMEM((images, width), f32),
            pltpu.VMEM((images, width), f32),
            pltpu.VMEM((groups, images, kdim), bf16),
            pltpu.VMEM((share, LANES), jnp.int32),
            pltpu.VMEM((share, groups * images), bf16),
            pltpu.VMEM((groups, images, LANES), f32),
            pltpu.VMEM((devices, images, LANES), f32),
            pltpu.VMEM((groups, images, kdim), bf16),
            pltpu.VMEM((groups, 1, LANES), f32),
            dma((10,)),
            dma,
            dma((images,)),
            dma((images,)),
            dma((groups,)),
            dma((groups,)),
            dma((groups,)),
            dma((devices,)),
            dma((devices,)),
            dma((groups,)),
            dma((devices,)),
            dma((groups,)),
        ],
        compiler_params=pltpu.CompilerParams(
            collective_id=0, has_side_effects=True, vmem_limit_bytes=56 * 1024 * 1024
        ),
        cost_estimate=pl.CostEstimate(flops=flops, bytes_accessed=2**24, transcendentals=2**22),
    )(
        jnp.transpose(patches, (1, 0, 2)),
        online_embeddings,
        ln1_gain,
        ln2_gain,
        final_norm_gain.reshape(1, width),
        w_qkv,
        w_out,
        w_fc1,
        w_fc2,
        w_head,
        queue,
        owner.reshape(1, groups * images),
        pointer,
    )
    return keys, loss.reshape(images), total.reshape(()), new_queue


def solution(mesh):
    placed = (
        P("dp", None, None),
        P("section", None),
        P("section", None, None),
        P("section", None, None),
        P("section", None),
        P("section", None, None),
        P("section", None, None),
        P(),
        P(),
        P("dp", None),
        P(("dp", "section"), None),
        P(),
        P("dp"),
    )
    return jax.shard_map(
        on_device,
        mesh=mesh,
        in_specs=placed,
        out_specs=(P("dp", None), P("dp"), P(), P(("dp", "section"), None)),
        check_vma=False,
    )
```

```python
import functools
import math

import jax
import jax.numpy as jnp
from jax import lax
from jax.experimental import pallas as pl
from jax.experimental.pallas import tpu as pltpu
from jax.sharding import PartitionSpec as P

HEAD_DIM = 64
LANES = 128
RAW_PARTS = 4
SHARPNESS = 0.2
f32 = jnp.float32
bf16 = jnp.bfloat16
MESH = pl.DeviceIdType.MESH


def layer_norm(values, gain):
    center = values - jnp.mean(values, axis=-1, keepdims=True)
    spread = jnp.mean(center * center, axis=-1, keepdims=True)
    return center * lax.rsqrt(spread + 1e-06) * gain


def rounded_up(value, step):
    return (value + step - 1) // step * step


def gelu(x):
    return 0.5 * x * (1.0 + lax.erf(x * math.sqrt(0.5)))


def dot(a, b):
    return jnp.dot(a, b, preferred_element_type=f32)


def dot_nt(a, b):
    return lax.dot_general(a, b, (((1,), (1,)), ((), ())), preferred_element_type=f32)


def column_loop(total, tile, body):
    for at in range(0, total, tile):
        body(at, tile)


def attend(qkv_buf, c_buf, toks, width):
    rows = c_buf.shape[0]
    pair = 2 * HEAD_DIM
    lane = lax.broadcasted_iota(jnp.int32, (rows, pair), 1)
    place = lax.broadcasted_iota(jnp.int32, (rows, pair), 0)
    first = lane < HEAD_DIM
    factor = math.log2(math.e) / math.sqrt(HEAD_DIM)
    one = (place < toks).astype(f32).astype(bf16)
    for at in range(0, width, pair):
        q = qkv_buf[:, pl.ds(at, pair)]
        zero = jnp.zeros_like(q)
        q_both = jnp.concatenate([jnp.where(first, q, zero), jnp.where(first, zero, q)], axis=0)
        scores = dot_nt(q_both, qkv_buf[:, pl.ds(width + at, pair)])
        peak = jnp.max(scores, axis=1, keepdims=True)
        expo = jnp.exp2((scores - peak) * factor)
        v_and_one = jnp.concatenate([qkv_buf[:, pl.ds(2 * width + at, pair)], one], axis=1)
        c = dot(expo.astype(bf16), v_and_one)
        above = jnp.where(first, c[:rows, :pair], c[rows:, :pair])
        below = jnp.where(first, c[:rows, pair:], c[rows:, pair:])
        c_buf[:, pl.ds(at, pair)] = (above / below).astype(bf16)


def encoder_kernel(
    sections,
    groups,
    toks,
    patches,
    online_hbm,
    gain_one_hbm,
    gain_two_hbm,
    gain_last_hbm,
    w_qkv,
    w_out,
    w_fc1,
    w_fc2,
    w_head,
    queue_hbm,
    owner_hbm,
    pointer,
    keys_out,
    loss_out,
    place_out,
    kept_out,
    v_qkv,
    v_out,
    v_fc1,
    v_fc2,
    v_head,
    raw,
    flat,
    came,
    leaving,
    a_buf,
    qkv_buf,
    c_buf,
    r_buf,
    u_buf,
    row_h,
    row_c,
    q_buf,
    stat_buf,
    stat_recv,
    key_buf,
    loss_buf,
    online,
    gain_one,
    gain_two,
    gain_last,
    queue,
    owner,
    scale_buf,
    negative_buf,
    weight_sem,
    small_sem,
    raw_sem,
    send_sem,
    recv_sem,
    q_send,
    q_recv,
    stat_send_sem,
    stat_recv_sem,
    key_send,
    key_recv,
    loss_send,
    loss_recv,
):
    me = lax.axis_index("section")
    group = lax.axis_index("dp")
    images, rows, width = came.shape
    hidden = v_fc1.shape[1]
    share, kdim = queue.shape
    last = sections - 1
    devices = groups * sections
    own = group * sections + me
    part = width // 2
    n_parts = 3 * width // part

    step_toks = (toks + RAW_PARTS - 1) // RAW_PARTS
    spans = [(at, min(step_toks, toks - at)) for at in range(0, toks, step_toks)]
    raw_loads = [
        pltpu.make_async_copy(
            patches.at[pl.ds(at, size)], raw.at[pl.ds(at, size)], raw_sem.at[i]
        )
        for i, (at, size) in enumerate(spans)
    ]
    small_loads = [
        pltpu.make_async_copy(source, target, small_sem.at[i])
        for i, (source, target) in enumerate(
            (
                (gain_one_hbm, gain_one),
                (gain_two_hbm, gain_two),
                (gain_last_hbm, gain_last),
                (online_hbm, online),
                (owner_hbm, owner),
                (queue_hbm, queue),
            )
        )
    ]
    qkv_loads = [
        pltpu.make_async_copy(
            w_qkv.at[0, :, pl.ds(i * part, part)],
            v_qkv.at[:, pl.ds(i * part, part)],
            weight_sem.at[i],
        )
        for i in range(n_parts)
    ]
    other_loads = [
        pltpu.make_async_copy(source, target, weight_sem.at[n_parts + i])
        for i, (source, target) in enumerate(
            ((w_out.at[0], v_out), (w_fc1.at[0], v_fc1), (w_fc2.at[0], v_fc2))
        )
    ]
    head_load = pltpu.make_async_copy(w_head, v_head, weight_sem.at[n_parts + 3])

    for load in small_loads[:-1]:
        load.start()

    @pl.when(me == 0)
    def _():
        for load in raw_loads:
            load.start()
        qkv_loads[0].start()

    @pl.when(me > 0)
    def _():
        small_loads[-1].start()
        for load in qkv_loads + other_loads:
            load.start()

    @pl.when(me == last)
    def _():
        head_load.start()

    barrier = pltpu.get_barrier_semaphore()

    @pl.loop(1, devices)
    def _(step):
        there = lax.rem(own + step, devices)
        pl.semaphore_signal(
            barrier,
            inc=1,
            device_id={"dp": there // sections, "section": lax.rem(there, sections)},
            device_id_type=MESH,
        )

    def query_copy(step):
        return pltpu.make_async_remote_copy(
            src_ref=online,
            dst_ref=q_buf.at[group],
            send_sem=q_send.at[step],
            recv_sem=q_recv.at[step],
            device_id={"dp": lax.rem(group + step, groups)},
            device_id_type=MESH,
        )

    def enter():
        small_loads[3].wait()
        pl.semaphore_wait(barrier, devices - 1)
        for step in range(1, groups):
            query_copy(step).start()

    def stat_copy(step):
        there = lax.rem(group + step, groups)
        return pltpu.make_async_remote_copy(
            src_ref=stat_buf.at[there],
            dst_ref=stat_recv.at[own],
            send_sem=stat_send_sem.at[step],
            recv_sem=stat_recv_sem.at[own],
            device_id={"dp": there, "section": last},
            device_id_type=MESH,
        )

    def side_work():
        small_loads[4].wait()
        small_loads[5].wait()
        for step in range(1, groups):
            query_copy(step).wait()
        q_buf[group] = online[...]
        queries = q_buf[...].astype(f32).reshape(groups * images, kdim).astype(bf16)
        scores = dot_nt(queries, queue[...]) / SHARPNESS
        peak = jnp.max(scores, axis=1, keepdims=True)
        total = jnp.sum(jnp.exp(scores - peak), axis=1, keepdims=True)
        stat = jnp.broadcast_to(peak + jnp.log(total), (groups * images, LANES))
        stat_buf[...] = stat.reshape(groups, images, LANES)

        for step in range(1, groups):
            stat_copy(step).start()

        @pl.when(me < last)
        def _():
            stat_copy(0).start()

        slot = (
            lax.broadcasted_iota(jnp.int32, (share, LANES), 0) + me * share - pointer[0]
        )
        inside = jnp.logical_and(slot >= 0, slot < images)
        code = jnp.where(inside, slot + group * images, -1)
        place_out[...] = (code[:, : groups * images] == owner[...]).astype(f32).astype(bf16)
        taken = jnp.concatenate([code] * (kdim // LANES), axis=1) >= 0
        kept_out[...] = jnp.where(taken, 0.0, queue[...].astype(f32)).astype(bf16)

        for step in range(1, groups):
            stat_copy(step).wait_send()

        @pl.when(me < last)
        def _():
            stat_copy(0).wait_send()

    def handing(image):
        return pltpu.make_async_remote_copy(
            src_ref=leaving.at[image],
            dst_ref=came.at[image],
            send_sem=send_sem.at[image],
            recv_sem=recv_sem.at[image],
            device_id={"section": jnp.minimum(me + 1, last)},
            device_id_type=MESH,
        )

    def extract(image):
        for tile in range(width // LANES):
            came[image, :, tile * LANES : (tile + 1) * LANES] = flat[
                tile, pl.ds(image, rows, stride=images), :
            ].astype(bf16)

    def centered(values, total, gain):
        middle = total * (1.0 / width)
        square = None
        for at in range(0, width, part // 2):
            columns = slice(at, at + part // 2)
            away = values[:, columns] - middle
            a_buf[:, columns] = (away * gain[:, columns]).astype(bf16)
            term = jnp.sum(away * away, axis=1, keepdims=True)
            square = term if square is None else square + term
        scale = lax.rsqrt(square * (1.0 / width) + 1e-06)
        scale_buf[...] = jnp.broadcast_to(scale, (rows, LANES))

    def scaled(values):
        return values * jnp.concatenate([scale_buf[...]] * (values.shape[1] // LANES), axis=1)

    def norm_one(image):
        values = came[image].astype(f32)
        centered(values, jnp.sum(values, axis=1, keepdims=True), gain_one)

    def block(image, starting, prefetched):
        if not prefetched:
            handing(image).wait_recv()
            norm_one(image)

        def qkv_part(at, tile):
            if starting:
                i = at // tile
                qkv_loads[i].wait()
                if i < 3:
                    other_loads[i].start()
                if i == 3:
                    small_loads[5].start()
            columns = pl.ds(at, tile)
            qkv_buf[:, columns] = scaled(dot(a_buf[...], v_qkv[:, columns])).astype(bf16)

        column_loop(3 * width, part, qkv_part)
        tail = toks // 16 * 16
        kept = lax.broadcasted_iota(jnp.int32, (rows - tail, width), 0) < toks - tail
        end = qkv_buf[tail:, 2 * width :]
        qkv_buf[tail:, 2 * width :] = jnp.where(kept, end, jnp.zeros_like(end))
        if starting:
            enter()

        attend(qkv_buf, c_buf, toks, width)
        if starting:
            other_loads[0].wait()

        sums = []

        def out_part(at, tile):
            columns = pl.ds(at, tile)
            r = came[image, :, columns].astype(f32) + dot(c_buf[...], v_out[:, columns])
            r_buf[:, columns] = r
            sums.append(jnp.sum(r, axis=1, keepdims=True))

        column_loop(width, part, out_part)
        centered(r_buf, sum(sums[1:], sums[0]), gain_two)
        if starting:
            other_loads[1].wait()

        def fc1_part(at, tile):
            columns = pl.ds(at, tile)
            u_buf[:, columns] = gelu(scaled(dot(a_buf[...], v_fc1[:, columns]))).astype(bf16)

        column_loop(hidden, part, fc1_part)
        if starting:
            other_loads[2].wait()

        def fc2_part(at, tile):
            columns = pl.ds(at, tile)
            leaving[image, :, columns] = (
                r_buf[:, columns] + dot(u_buf[...], v_fc2[:, columns])
            ).astype(bf16)

        column_loop(width, part, fc2_part)
        if prefetched:
            following = jnp.minimum(image + 1, images - 1)
            extract(following)
            norm_one(following)
        handing(image).start()

    def class_row(image):
        handing(image).wait_recv()
        row_h[pl.ds(image, 1), :] = came[image, 0:16, :].astype(f32)[0:1, :]
        a_buf[...] = layer_norm(came[image].astype(f32), gain_one[...]).astype(bf16)
        q = dot(a_buf[0:16, :], v_qkv[:, 0:width]).astype(bf16).astype(f32)[0:1, :]

        def kv_part(at, tile):
            columns = pl.ds(width + at, tile)
            qkv_buf[:, columns] = dot(a_buf[...], v_qkv[:, columns]).astype(bf16)

        column_loop(2 * width, part, kv_part)
        heads = width // HEAD_DIM
        head = lax.broadcasted_iota(jnp.int32, (heads, width), 0)
        lane = lax.broadcasted_iota(jnp.int32, (heads, width), 1)
        mine = lane // HEAD_DIM == head
        spread = jnp.where(mine, jnp.broadcast_to(q, (heads, width)), 0.0).astype(bf16)
        scores = dot_nt(spread, qkv_buf[:, width : 2 * width]) / math.sqrt(HEAD_DIM)
        place = lax.broadcasted_iota(jnp.int32, (heads, rows), 1)
        scores = jnp.where(place < toks, scores, -jnp.inf)
        expo = jnp.exp(scores - jnp.max(scores, axis=1, keepdims=True))
        p = (expo / jnp.sum(expo, axis=1, keepdims=True)).astype(bf16)
        c = dot(p, qkv_buf[:, 2 * width :])
        row_c[pl.ds(image, 1), :] = jnp.sum(jnp.where(mine, c, 0.0), axis=0, keepdims=True)

    def key_copy(step):
        there = lax.rem(own + step, devices)
        return pltpu.make_async_remote_copy(
            src_ref=key_buf.at[group],
            dst_ref=key_buf.at[group],
            send_sem=key_send.at[step],
            recv_sem=key_recv.at[group],
            device_id={"dp": there // sections, "section": lax.rem(there, sections)},
            device_id_type=MESH,
        )

    def loss_copy(step):
        there = lax.rem(own + step, devices)
        return pltpu.make_async_remote_copy(
            src_ref=loss_buf.at[group],
            dst_ref=loss_buf.at[group],
            send_sem=loss_send.at[step],
            recv_sem=loss_recv.at[group],
            device_id={"dp": there // sections, "section": lax.rem(there, sections)},
            device_id_type=MESH,
        )

    def finish_keys():
        r = row_h[...] + dot(row_c[...].astype(bf16), v_out[...])
        u = gelu(dot(layer_norm(r, gain_two[...]).astype(bf16), v_fc1[...])).astype(bf16)
        h = (r + dot(u, v_fc2[...])).astype(bf16).astype(f32)
        z = dot(layer_norm(h, gain_last[...]).astype(bf16), v_head[...])
        keys = (z * lax.rsqrt(1.0 + jnp.sum(z * z, axis=1, keepdims=True))).astype(bf16)
        key_buf[group] = keys

        for step in range(1, devices):
            key_copy(step).start()

        negative = negative_buf[...]
        positive = jnp.broadcast_to(
            jnp.sum(online[...].astype(f32) * keys.astype(f32), axis=1, keepdims=True) / SHARPNESS,
            (images, LANES),
        )
        larger = jnp.maximum(negative, positive)
        loss = (
            larger + jnp.log(jnp.exp(negative - larger) + jnp.exp(positive - larger)) - positive
        )
        row = lax.broadcasted_iota(jnp.int32, (images, LANES), 0)
        lane = lax.broadcasted_iota(jnp.int32, (images, LANES), 1)
        loss_buf[group] = jnp.sum(jnp.where(row == lane, loss, 0.0), axis=0, keepdims=True)

        for step in range(1, devices):
            loss_copy(step).start()

    @pl.when(me == 0)
    def _():
        for i, (at, size) in enumerate(spans):
            raw_loads[i].wait()
            qkv_loads[i + 1].start()
            for tile in range(width // LANES):
                columns = slice(tile * LANES, (tile + 1) * LANES)
                flat[tile, at * images : (at + size) * images, :] = (
                    raw[at : at + size, :, columns].astype(f32).reshape(size * images, LANES)
                )
        for load in qkv_loads[len(spans) + 1 :]:
            load.start()
        for tile in range(width // LANES):
            flat[tile, toks * images :, :] = flat[tile, 0 : (rows - toks) * images, :]
        for load in small_loads[0:3]:
            load.wait()
        extract(0)
        norm_one(0)
        block(0, True, True)

        @pl.loop(1, images)
        def _(image):
            block(image, False, True)

        side_work()

    @pl.when(me > 0)
    def _():
        enter()
        side_work()
        for load in small_loads[0:3]:
            load.wait()
        for load in qkv_loads + other_loads:
            load.wait()

    @pl.when(jnp.logical_and(me > 0, me < last))
    def _():
        @pl.loop(0, images)
        def _(image):
            block(image, False, False)

    @pl.when(me == last)
    def _():
        head_load.wait()

        @pl.loop(0, images - 1)
        def _(image):
            class_row(image)

        @pl.loop(1, devices)
        def _(step):
            there = lax.rem(own + step, devices)
            pltpu.make_async_remote_copy(
                src_ref=stat_buf.at[group],
                dst_ref=stat_recv.at[there],
                send_sem=stat_send_sem.at[0],
                recv_sem=stat_recv_sem.at[there],
                device_id={"dp": group, "section": last},
                device_id_type=MESH,
            ).wait_recv()

        stat_recv[own] = stat_buf[group]
        stats = stat_recv[...]
        top = jnp.max(stats, axis=0)
        negative_buf[...] = top + jnp.log(jnp.sum(jnp.exp(stats - top[None]), axis=0))
        class_row(images - 1)
        finish_keys()

    for step in range(groups):
        there = lax.rem(group + step, groups)

        def arrived():
            pltpu.make_async_remote_copy(
                src_ref=key_buf.at[there],
                dst_ref=key_buf.at[there],
                send_sem=key_send.at[0],
                recv_sem=key_recv.at[there],
                device_id={"section": last},
                device_id_type=MESH,
            ).wait_recv()
            pltpu.make_async_remote_copy(
                src_ref=loss_buf.at[there],
                dst_ref=loss_buf.at[there],
                send_sem=loss_send.at[0],
                recv_sem=loss_recv.at[there],
                device_id={"section": last},
                device_id_type=MESH,
            ).wait_recv()

        if step == 0:
            pl.when(me < last)(arrived)
        else:
            arrived()

    keys_out[...] = key_buf[...]
    loss_out[...] = loss_buf[...]

    @pl.when(me < last)
    def _():
        @pl.loop(0, images)
        def _(image):
            handing(image).wait_send()

    @pl.when(me == last)
    def _():
        @pl.loop(1, devices)
        def _(step):
            key_copy(step).wait_send()
            loss_copy(step).wait_send()


def finish_kernel(groups, all_keys, losses, place, kept, keys_out, loss_out, total_out, queue_out):
    group = lax.axis_index("dp")
    images, kdim = keys_out.shape
    every_key = all_keys[...].astype(f32).reshape(groups * images, kdim).astype(bf16)
    queue_out[...] = (dot(place[...], every_key) + kept[...].astype(f32)).astype(bf16)
    keys_out[...] = all_keys[group]
    loss_out[...] = losses[group][:, 0:images]
    total = jnp.sum(losses[...], axis=0)
    total_out[...] = jnp.sum(total, axis=1, keepdims=True) / (groups * images)


def on_device(
    patches,
    ln1_gain,
    w_qkv,
    w_out,
    ln2_gain,
    w_fc1,
    w_fc2,
    final_norm_gain,
    w_head,
    online_embeddings,
    queue,
    owner,
    pointer,
):
    sections = lax.axis_size("section")
    groups = lax.axis_size("dp")
    devices = sections * groups
    images, toks, width = patches.shape
    rows = rounded_up(toks, 16)
    hidden = w_fc1.shape[2]
    share, kdim = queue.shape
    in_vmem = pl.BlockSpec(memory_space=pltpu.VMEM)
    in_smem = pl.BlockSpec(memory_space=pltpu.SMEM)
    hbm = pl.BlockSpec(memory_space=pltpu.HBM)
    dma = pltpu.SemaphoreType.DMA
    flops = 2 * images * toks * (4 * width * width + 2 * width * hidden)
    all_keys, losses, place, kept = pl.pallas_call(
        functools.partial(encoder_kernel, sections, groups, toks),
        out_shape=(
            jax.ShapeDtypeStruct((groups, images, kdim), bf16),
            jax.ShapeDtypeStruct((groups, 1, LANES), f32),
            jax.ShapeDtypeStruct((share, groups * images), bf16),
            jax.ShapeDtypeStruct((share, kdim), bf16),
        ),
        in_specs=[hbm] * 12 + [in_smem],
        out_specs=(in_vmem,) * 4,
        scratch_shapes=[
            pltpu.VMEM((width, 3 * width), bf16),
            pltpu.VMEM((width, width), bf16),
            pltpu.VMEM((width, hidden), bf16),
            pltpu.VMEM((hidden, width), bf16),
            pltpu.VMEM((width, kdim), bf16),
            pltpu.VMEM((toks, images, width), bf16),
            pltpu.VMEM((width // LANES, rows * images, LANES), f32),
            pltpu.VMEM((images, rows, width), bf16),
            pltpu.VMEM((images, rows, width), bf16),
            pltpu.VMEM((rows, width), bf16),
            pltpu.VMEM((rows, 3 * width), bf16),
            pltpu.VMEM((rows, width), bf16),
            pltpu.VMEM((rows, width), f32),
            pltpu.VMEM((rows, hidden), bf16),
            pltpu.VMEM((images, width), f32),
            pltpu.VMEM((images, width), f32),
            pltpu.VMEM((groups, images, kdim), bf16),
            pltpu.VMEM((groups, images, LANES), f32),
            pltpu.VMEM((devices, images, LANES), f32),
            pltpu.VMEM((groups, images, kdim), bf16),
            pltpu.VMEM((groups, 1, LANES), f32),
            pltpu.VMEM((images, kdim), bf16),
            pltpu.VMEM((1, width), f32),
            pltpu.VMEM((1, width), f32),
            pltpu.VMEM((1, width), f32),
            pltpu.VMEM((share, kdim), bf16),
            pltpu.VMEM((1, groups * images), jnp.int32),
            pltpu.VMEM((rows, LANES), f32),
            pltpu.VMEM((images, LANES), f32),
            dma((10,)),
            dma((6,)),
            dma((RAW_PARTS,)),
            dma((images,)),
            dma((images,)),
            dma((groups,)),
            dma((groups,)),
            dma((groups,)),
            dma((devices,)),
            dma((devices,)),
            dma((groups,)),
            dma((devices,)),
            dma((groups,)),
        ],
        compiler_params=pltpu.CompilerParams(
            collective_id=0, has_side_effects=True, vmem_limit_bytes=48 * 1024 * 1024
        ),
        cost_estimate=pl.CostEstimate(flops=flops, bytes_accessed=2**24, transcendentals=2**22),
    )(
        *(
            pltpu.with_memory_space_constraint(array, pltpu.HBM)
            for array in (
                jnp.transpose(patches, (1, 0, 2)),
                online_embeddings,
                ln1_gain,
                ln2_gain,
                final_norm_gain.reshape(1, width),
                w_qkv,
                w_out,
                w_fc1,
                w_fc2,
                w_head,
                queue,
                owner.reshape(1, groups * images),
            )
        ),
        pointer,
    )
    keys, loss, total, new_queue = pl.pallas_call(
        functools.partial(finish_kernel, groups),
        out_shape=(
            jax.ShapeDtypeStruct((images, kdim), bf16),
            jax.ShapeDtypeStruct((1, images), f32),
            jax.ShapeDtypeStruct((1, 1), f32),
            jax.ShapeDtypeStruct((share, kdim), bf16),
        ),
        in_specs=[in_vmem] * 4,
        out_specs=(in_vmem,) * 4,
        compiler_params=pltpu.CompilerParams(vmem_limit_bytes=4 * 1024 * 1024),
    )(all_keys, losses, place, kept)
    return keys, loss.reshape(images), total.reshape(()), new_queue


def solution(mesh):
    placed = (
        P("dp", None, None),
        P("section", None),
        P("section", None, None),
        P("section", None, None),
        P("section", None),
        P("section", None, None),
        P("section", None, None),
        P(),
        P(),
        P("dp", None),
        P(("dp", "section"), None),
        P(),
        P("dp"),
    )
    return jax.shard_map(
        on_device,
        mesh=mesh,
        in_specs=placed,
        out_specs=(P("dp", None), P("dp"), P(), P(("dp", "section"), None)),
        check_vma=False,
    )
```
